32 devices in a mesh: pts: 8 (over z, y), cam: 4 (over x, core).
Axes of the slice: x: 2, y: 2, z: 4, core: 2. Of those that a mesh axis runs over, the one named last changes fastest.
Arguments:
- feat_res: bfloat16 [16, 128, 16384], P(None, None, ('pts', 'cam')), may hold values from -6 to 6
- feat_grad: bfloat16 [2, 16, 128, 16384], P(None, None, None, ('pts', 'cam')), may hold values from -0.125 to 0.125
- cam_jac: float32 [2, 6, 16384], P(None, None, ('pts', 'cam')), may hold values from -6 to 6
- pt_jac: float32 [2, 3, 16384], P(None, None, ('pts', 'cam')), may hold values from -6 to 6
- obs_camera: int32 [16384], P(('pts', 'cam')), may hold values from 0 to 255
- point_counts: int32 [32, 128], P(('pts', 'cam')), may hold values from 1 to 16, 512 in all within a row
Outputs:
- camera_step: float32 [6, 256], replicated
- point_step: float32 [3, 4096], P(None, ('pts', 'cam'))
The draws below stay inside these ranges and needn't reach their ends.
Inputs may be any that keep to these rules, and one draw needn't show every extreme that they name: Each row of point_counts sums to 512, so every point's observations lie on the device that holds the point.
All inputs are finite; a program needn't handle non-finite values.
Results may differ from the reference program's by a relative error of at most 0.0003.
Values sent between devices are 32-bit elements; how exact they have to be, the bound alone decides.
A program may use at most 128 MiB of HBM per device.

```python
import math
import jax
import jax.numpy as jnp
import numpy as np
from jax import lax

PIX = 16
CH = 128
PTS_DEV = 128
OBS_PER = 4
MOST_OBS = 16
ITERS = 4
CAMS = 256
POINTS = 4096
OBS = 16384
N_PTS = 8
N_CAM = 4


def touch_ends(entries, key, smallest, top_value):
    shape = entries.shape
    spot = [jax.random.randint(jax.random.fold_in(key, axis), (), 0, shape[axis]) for axis in range(len(shape))]
    entries = entries.at[tuple(spot)].set(smallest)
    longest = shape.index(max(shape))
    spot[longest] = (spot[longest] + 1) % shape[longest]
    return entries.at[tuple(spot)].set(top_value)


def shard_levels(rng, extent, cuts, least, largest):
    def one(dim, parts):
        steps = jax.random.uniform(jax.random.fold_in(jax.random.fold_in(rng, 6), dim), (parts,), jnp.float32, least / len(cuts), largest / len(cuts))
        return jnp.repeat(jnp.exp(steps), extent[dim] // parts).reshape((-1,) + (1,) * (len(extent) - dim - 1))

    level = one(*cuts[0])
    for cut in cuts[1:]:
        level = level * one(*cut)
    return level


def rank_table(number_of, slope):
    weights = [(1 << 20) // math.isqrt(standing ** slope) + 1 for standing in range(1, number_of + 1)]
    spread = 1 + sum(weights) // (1 << 30)
    return np.cumsum(np.array([max(1, weight // spread) for weight in weights]))


def skewed_ids(own_key, shape, number_of, lean):
    table = rank_table(number_of, lean)
    pick = jax.random.randint(jax.random.fold_in(own_key, 1), shape, 0, int(table[number_of - 1]))
    standing = jnp.searchsorted(jnp.asarray(table, jnp.int32), pick, side="right")
    return jax.random.permutation(jax.random.fold_in(own_key, 2), number_of)[standing].astype(jnp.int32)


def length_profile(number_of, total, most, slope):
    loads = [(1 << 20) // math.isqrt(rank ** slope) + 1 for rank in range(2, number_of + 1)]
    rest, given = total - most - (number_of - 1), [1] * (number_of - 1)
    while rest > 0:
        free = [i for i in range(number_of - 1) if given[i] < most]
        mass, left = sum([loads[i] for i in free]), rest
        for i in free:
            more = min(most - given[i], max(1, left * loads[i] // mass), rest)
            given[i] = given[i] + more
            rest = rest - more
    return np.array([most] + given)


def ragged_sizes(rng, number_of, total, most, skew):
    if number_of == 2:
        one = jax.random.randint(rng, (), max(1, total - most), min(most, total - 1) + 1)
        return jnp.stack([one, total - one])
    sizes = jnp.asarray(length_profile(number_of, total, most, skew), jnp.int32)
    pairs = (number_of - 1) // 2
    source_of, sink = sizes[1:1 + 2 * pairs:2], sizes[2:2 + 2 * pairs:2]
    margin = jnp.minimum(source_of - 1, most - sink)
    passed = jax.random.randint(jax.random.fold_in(rng, 1), (pairs,), 0, 1 << 20) % (margin + 1)
    sizes = sizes.at[1:1 + 2 * pairs:2].set(source_of - passed).at[2:2 + 2 * pairs:2].set(sink + passed)
    return sizes[jax.random.permutation(jax.random.fold_in(rng, 2), number_of)]


def normal_values(stream_key, shape, width, most, split=(), held_as=jnp.bfloat16):
    array = jax.random.normal(stream_key, shape, jnp.float32) * width
    if len(split) > 0:
        array = shard_levels(stream_key, shape, split, -0.22, 0.18) * array
    return jnp.clip(array, min=-most, max=most).astype(held_as)


def setup_inputs(seed: int = 0) -> dict:
    streams_of = jax.random.split(jax.random.key(seed), 7)
    return {
        "feat_res": normal_values(streams_of[0], (PIX, CH, OBS), 1.0, 6.0, ((2, 32),)),
        "feat_grad": normal_values(streams_of[1], (2, PIX, CH, OBS), (PIX * CH) ** -0.5, 0.125, ((3, 32),)),
        "cam_jac": normal_values(streams_of[2], (2, 6, OBS), 1.0, 6.0, ((2, 32),), jnp.float32),
        "pt_jac": normal_values(streams_of[3], (2, 3, OBS), 1.0, 6.0, ((2, 32),), jnp.float32),
        "obs_camera": touch_ends(skewed_ids(streams_of[4], (OBS,), CAMS, 2), jax.random.fold_in(streams_of[4], 3), 0, CAMS - 1).astype(jnp.int32),
        "point_counts": jax.vmap(lambda own: ragged_sizes(own, PTS_DEV, OBS_PER * PTS_DEV, MOST_OBS, 2))(jax.random.split(streams_of[5], (N_PTS * N_CAM))).reshape((N_PTS * N_CAM, PTS_DEV)).astype(jnp.int32),
    }


damping = 1.0
highest = lax.Precision.HIGHEST

def feature_terms(residual, gradient):
    residual = residual.astype(jnp.float32)
    gradient = gradient.astype(jnp.float32)
    energy = jnp.einsum('pcn,pcn->n', residual, residual, precision=highest)
    moment = jnp.einsum('apcn,bpcn->abn', gradient, gradient, precision=highest)
    pulled = jnp.einsum('apcn,pcn->an', gradient, residual, precision=highest)
    weight = 1.0 / (1.0 + energy / (residual.shape[0] * residual.shape[1]))
    return (moment * weight, pulled * weight)

def segment_total(values, indices, segments):
    return jax.ops.segment_sum(values.T, indices, num_segments=segments).T

def cholesky_rows(matrix, dimension):
    factor = [[None] * dimension for position in range(dimension)]
    for column in range(dimension):
        pivot_value = matrix[column][column]
        for earlier in range(column):
            pivot_value = pivot_value - factor[column][earlier] * factor[column][earlier]
        factor[column][column] = jnp.sqrt(pivot_value)
        for lower_row in range(column + 1, dimension):
            element = matrix[lower_row][column]
            for earlier in range(column):
                element = element - factor[lower_row][earlier] * factor[column][earlier]
            factor[lower_row][column] = element / factor[column][column]
    return factor

def take_factor(factor, indices):
    picked = []
    for row_list in factor:
        picked.append([None if element is None else element[indices] for element in row_list])
    return picked

def cholesky_solve(factor, right_side):
    dimension = len(factor)
    forward = []
    for column in range(dimension):
        element = right_side[column]
        for earlier in range(column):
            element = element - factor[column][earlier] * forward[earlier]
        forward.append(element / factor[column][column])
    backward = [None] * dimension
    for column in reversed(range(dimension)):
        element = forward[column]
        for latter in range(column + 1, dimension):
            element = element - factor[latter][column] * backward[latter]
        backward[column] = element / factor[column][column]
    return jnp.stack(backward)

def point_system(moment, pulled, pt_jac, point_ids, segments):
    weighted = jnp.einsum('abn,bjn->ajn', moment, pt_jac, precision=highest)
    blocks = jnp.einsum('ain,ajn->ijn', pt_jac, weighted, precision=highest)
    point_force = jnp.einsum('ain,an->in', pt_jac, pulled, precision=highest)
    summed = segment_total(jnp.concatenate([blocks.reshape(9, -1), point_force]), point_ids, segments)
    hessian = summed[:9].reshape(3, 3, -1) + damping * jnp.eye(3, dtype=jnp.float32)[:, :, None]
    return (cholesky_rows(hessian, 3), summed[9:])

def camera_terms(moment, pulled, cam_jac, pt_jac, point_factor, point_force, point_ids):
    local_factor = take_factor(point_factor, point_ids)
    toward = jnp.einsum('abn,bjn->ajn', moment, cam_jac, precision=highest)
    camera_block = jnp.einsum('ain,ajn->ijn', cam_jac, toward, precision=highest)
    coupling = jnp.einsum('ain,ajn->ijn', pt_jac, toward, precision=highest)
    solved = cholesky_solve(local_factor, coupling)
    reduced = camera_block - jnp.einsum('kin,kjn->ijn', coupling, solved, precision=highest)
    point_shift = cholesky_solve(point_factor, point_force)[:, point_ids]
    pointward = jnp.einsum('abn,bjn->ajn', moment, pt_jac, precision=highest)
    leftover = pulled - jnp.einsum('ajn,jn->an', pointward, point_shift, precision=highest)
    gradient = jnp.einsum('ain,an->in', cam_jac, leftover, precision=highest)
    return jnp.concatenate([reduced.reshape(36, -1), gradient])

def camera_image(values, moment, cam_jac, pt_jac, point_factor, point_ids, slot_ids, point_total, slot_total):
    at_obs = values[:, slot_ids]
    projected = jnp.einsum('ajn,jn->an', cam_jac, at_obs, precision=highest)
    pushed = jnp.einsum('abn,bn->an', moment, projected, precision=highest)
    gathered = segment_total(jnp.einsum('ain,an->in', pt_jac, pushed, precision=highest), point_ids, point_total)
    answer = cholesky_solve(point_factor, gathered)[:, point_ids]
    remain = projected - jnp.einsum('ajn,jn->an', pt_jac, answer, precision=highest)
    image_terms = jnp.einsum('ain,abn,bn->in', cam_jac, moment, remain, precision=highest)
    return segment_total(image_terms, slot_ids, slot_total)

def point_update(values, moment, pulled, cam_jac, pt_jac, point_factor, point_ids, slot_ids, point_total):
    projected = jnp.einsum('ajn,jn->an', cam_jac, values[:, slot_ids], precision=highest)
    pushed = pulled + jnp.einsum('abn,bn->an', moment, projected, precision=highest)
    point_force = segment_total(jnp.einsum('ain,an->in', pt_jac, pushed, precision=highest), point_ids, point_total)
    return -cholesky_solve(point_factor, point_force)

def camera_factor_of(camera_sums):
    matrix = camera_sums[:36].reshape(6, 6, -1) + damping * jnp.eye(6, dtype=jnp.float32)[:, :, None]
    return cholesky_rows(matrix, 6)

def reference(feat_res, feat_grad, cam_jac, pt_jac, obs_camera, point_counts):
    devices = N_PTS * N_CAM
    block_rows = feat_res.shape[2] // devices

    def one_block(position):
        first_row = position * block_rows
        return feature_terms(lax.dynamic_slice_in_dim(feat_res, first_row, block_rows, 2), lax.dynamic_slice_in_dim(feat_grad, first_row, block_rows, 3))
    moment, pulled = lax.map(one_block, jnp.arange(devices, dtype=jnp.int32))
    moment = jnp.transpose(moment, (1, 2, 0, 3)).reshape(2, 2, -1)
    pulled = jnp.transpose(pulled, (1, 0, 2)).reshape(2, -1)
    observations = pulled.shape[1]
    ends = jnp.cumsum(point_counts.reshape(-1)).astype(jnp.int32)
    point_ids = jnp.searchsorted(ends, jnp.arange(observations, dtype=jnp.int32), side='right').astype(jnp.int32)
    slot_ids = obs_camera
    point_factor, point_force = point_system(moment, pulled, pt_jac, point_ids, POINTS)
    camera_sums = segment_total(camera_terms(moment, pulled, cam_jac, pt_jac, point_factor, point_force, point_ids), slot_ids, CAMS)
    camera_factor = camera_factor_of(camera_sums)
    remaining = -camera_sums[36:]
    precond = cholesky_solve(camera_factor, remaining)
    direction = precond
    progress = jnp.sum(remaining * precond)
    solution = jnp.zeros_like(remaining)
    for step_index in range(ITERS):
        image = camera_image(direction, moment, cam_jac, pt_jac, point_factor, point_ids, slot_ids, POINTS, CAMS) + damping * direction
        alpha_value = progress / jnp.sum(direction * image)
        solution = solution + alpha_value * direction
        remaining = remaining - alpha_value * image
        precond = cholesky_solve(camera_factor, remaining)
        renewed = jnp.sum(remaining * precond)
        direction = precond + renewed / progress * direction
        progress = renewed
    point_step = point_update(solution, moment, pulled, cam_jac, pt_jac, point_factor, point_ids, slot_ids, POINTS)
    return (solution, point_step)
```

```python
import jax
import jax.numpy as jnp
from jax import lax
from jax.experimental import pallas as pl
from jax.experimental.pallas import tpu as pltpu
from jax.sharding import PartitionSpec as P

CAM_DEV = 8
ITERS = 4
CHUNK = 4
AXES = ("cam", "pts")
MESH = pl.DeviceIdType.MESH
f32 = jnp.float32
bf16 = jnp.bfloat16


def feature_kernel(res_ref, grad_ref, out_ref, acc_ref):
    step = pl.program_id(0)
    pixels, channels, width = res_ref.shape
    slabs = channels // 16

    @pl.when(step == 0)
    def _():
        acc_ref[...] = jnp.zeros_like(acc_ref)

    def fold(value):
        return value[:8] + value[8:]

    def pixel(index, carry):
        sums = list(carry)
        for slab in range(slabs):
            rows = slice(16 * slab, 16 * slab + 16)
            r = res_ref[index, rows, :].astype(f32)
            gx = grad_ref[0, index, rows, :].astype(f32)
            gy = grad_ref[1, index, rows, :].astype(f32)
            for spot, (one, two) in enumerate(
                ((r, r), (gx, gx), (gx, gy), (gy, gy), (gx, r), (gy, r))
            ):
                sums[spot] = sums[spot] + fold(one * two)
        return tuple(sums)

    sums = lax.fori_loop(0, pixels, pixel, tuple(acc_ref[spot] for spot in range(6)))
    for spot in range(6):
        acc_ref[spot] = sums[spot]

    @pl.when(step == pl.num_programs(0) - 1)
    def _():
        whole = [jnp.sum(acc_ref[spot], axis=0, keepdims=True) for spot in range(6)]
        weight = 1.0 / (1.0 + whole[0] / (pixels * pl.num_programs(0) * channels))
        rows = [value * weight for value in whole[1:]]
        out_ref[...] = jnp.concatenate(rows + [jnp.zeros((3, width), f32)], axis=0)


def features(feat_res, feat_grad):
    pixels, channels, width = feat_res.shape
    return pl.pallas_call(
        feature_kernel,
        grid=(pixels // CHUNK,),
        in_specs=[
            pl.BlockSpec((CHUNK, channels, width), lambda i: (i, 0, 0)),
            pl.BlockSpec((2, CHUNK, channels, width), lambda i: (0, i, 0, 0)),
        ],
        out_specs=pl.BlockSpec((8, width), lambda i: (0, 0)),
        out_shape=jax.ShapeDtypeStruct((8, width), f32),
        scratch_shapes=[pltpu.VMEM((6, 8, width), f32)],
    )(feat_res, feat_grad)


def exact_dot(value, table, contract):
    rows = value.shape[0]
    high = value.astype(bf16).astype(f32)
    rest = value - high
    middle = rest.astype(bf16).astype(f32)
    pieces = jnp.concatenate([high, middle, rest - middle], axis=0).astype(bf16)
    product = lax.dot_general(
        pieces, table, (((1,), (contract,)), ((), ())), preferred_element_type=f32
    )
    return (product[:rows] + product[rows : 2 * rows]) + product[2 * rows :]


def pad_rows(rows, total):
    have = sum(row.shape[0] for row in rows)
    return jnp.concatenate(rows + [jnp.zeros((total - have, rows[0].shape[1]), f32)], axis=0)


def add_rows(value):
    return jnp.sum(value, axis=0, keepdims=True)


def add_all(value):
    return jnp.sum(jnp.sum(value, axis=0, keepdims=True), axis=1, keepdims=True)


def table_of(mask):
    return jnp.where(mask, 1.0, 0.0).astype(bf16)


def solver_kernel(sizes, feat_ref, cam_ref, pt_ref, id_ref, count_ref, step_ref, point_ref, *scratch):
    places = {axis: lax.axis_index(axis) for axis in AXES}
    buffers, semaphores = scratch[: 2 * (ITERS + 1)], scratch[2 * (ITERS + 1) :]
    cameras, points, width = step_ref.shape[1], point_ref.shape[1], id_ref.shape[1]

    barrier = pltpu.get_barrier_semaphore()
    for axis in AXES:
        for away in range(1, sizes[axis]):
            other = lax.rem(places[axis] + away, sizes[axis])
            pl.semaphore_signal(barrier, inc=1, device_id={axis: other}, device_id_type=MESH)

    def all_reduce(value, turn):
        for level, axis in enumerate(AXES):
            me, size = places[axis], sizes[axis]
            held = buffers[2 * turn + level]
            sent, arrived = semaphores[2 * level], semaphores[2 * level + 1]
            held[me] = value
            copies = []
            for away in range(1, size):
                copies.append(
                    pltpu.make_async_remote_copy(
                        src_ref=held.at[me],
                        dst_ref=held.at[me],
                        send_sem=sent.at[turn, away - 1],
                        recv_sem=arrived.at[turn, away - 1],
                        device_id={axis: lax.rem(me + away, size)},
                        device_id_type=MESH,
                    )
                )
                copies[-1].start()
            for copy in copies:
                copy.wait()
            value = held[0]
            for position in range(1, size):
                value = value + held[position]
        return value

    cam_table = table_of(lax.broadcasted_iota(jnp.int32, (cameras, width), 0) == id_ref[...])
    counts = count_ref[...].astype(f32)
    upper = lax.broadcasted_iota(jnp.int32, (points, points), 0)
    lower = lax.broadcasted_iota(jnp.int32, (points, points), 1)
    ends = jnp.sum(jnp.where(lower <= upper, counts, 0.0), axis=1, keepdims=True)
    starts = jnp.sum(jnp.where(lower < upper, counts, 0.0), axis=1, keepdims=True)
    spot = lax.broadcasted_iota(jnp.int32, (points, width), 1).astype(f32)
    member = (spot >= starts) & (spot < ends)
    first_table = table_of(spot == starts)
    start_row = add_rows(jnp.where(member, starts, 0.0))
    end_row = add_rows(jnp.where(member, ends, 0.0))
    line = lax.broadcasted_iota(jnp.int32, (width, width), 0).astype(f32)
    same_table = table_of((line >= start_row) & (line < end_row))

    m00, m01, m11, p0, p1 = (feat_ref[row : row + 1, :] for row in range(5))
    jc = [pad_rows([cam_ref[axis]], 8) for axis in range(2)]
    jp = [[pt_ref[axis, row : row + 1, :] for row in range(3)] for axis in range(2)]

    mjp = [
        [m00 * jp[0][k] + m01 * jp[1][k] for k in range(3)],
        [m01 * jp[0][k] + m11 * jp[1][k] for k in range(3)],
    ]
    pairs = [(0, 0), (1, 0), (2, 0), (1, 1), (2, 1), (2, 2)]
    rows = [jp[0][i] * mjp[0][j] + jp[1][i] * mjp[1][j] for i, j in pairs]
    rows += [jp[0][k] * p0 + jp[1][k] * p1 for k in range(3)]
    summed = exact_dot(pad_rows(rows, 16), same_table, 0)
    h00, h10, h20, h11, h21, h22, g0, g1, g2 = (summed[row : row + 1] for row in range(9))
    i0 = 1.0 / jnp.sqrt(h00 + 1.0)
    l10, l20 = h10 * i0, h20 * i0
    i1 = 1.0 / jnp.sqrt((h11 + 1.0) - l10 * l10)
    l21 = (h21 - l20 * l10) * i1
    i2 = 1.0 / jnp.sqrt((h22 + 1.0) - l20 * l20 - l21 * l21)

    def forward(a, b, c):
        a = a * i0
        b = (b - l10 * a) * i1
        return a, b, (c - l20 * a - l21 * b) * i2

    mjc = [m00 * jc[0] + m01 * jc[1], m01 * jc[0] + m11 * jc[1]]
    couple = forward(*(jp[0][k] * mjc[0] + jp[1][k] * mjc[1] for k in range(3)))
    force = forward(g0, g1, g2)

    terms = []
    for row in range(6):
        cut = slice(row, row + 1)
        term = jc[0][cut] * mjc[0] + jc[1][cut] * mjc[1]
        for k in range(3):
            term = term - couple[k][cut] * couple[k]
        terms.append(term)
    term = jc[0] * p0 + jc[1] * p1
    for k in range(3):
        term = term - couple[k] * force[k]
    terms.append(term)
    local = exact_dot(jnp.concatenate(terms, axis=0), cam_table, 1)
    packed = [local[8 * row + row : 8 * row + 6] for row in range(6)] + [local[48:54]]
    packed = pad_rows(packed, 32)

    pl.semaphore_wait(barrier, sum(sizes[axis] - 1 for axis in AXES))
    total = all_reduce(packed, 0)

    offsets = [0, 6, 11, 15, 18, 20, 21]

    def entry(i, j):
        low, high = min(i, j), max(i, j)
        at = offsets[low] + high - low
        return total[at : at + 1]

    level = lax.broadcasted_iota(jnp.int32, (8, cameras), 0)
    inverse = [
        pad_rows([entry(i, j) for j in range(6)], 8) + jnp.where(level == i, 1.0, 0.0)
        for i in range(6)
    ]
    for k in range(6):
        scale = 1.0 / inverse[k][k : k + 1]
        pivot = jnp.where(level == k, scale, inverse[k] * scale)
        for i in range(6):
            if i != k:
                factor = inverse[i][k : k + 1]
                inverse[i] = jnp.where(level == k, 0.0, inverse[i]) - factor * pivot
        inverse[k] = pivot

    def precondition(value):
        answer = inverse[0] * value[0:1]
        for j in range(1, 6):
            answer = answer + inverse[j] * value[j : j + 1]
        return answer

    remaining = -pad_rows([total[21:27]], 8)
    direction = precondition(remaining)
    progress = add_all(remaining * direction)
    solution = jnp.zeros_like(direction)
    reached = list(force)
    for turn in range(1, ITERS + 1):
        at_obs = exact_dot(direction, cam_table, 0)
        projected = [add_rows(jc[axis] * at_obs) for axis in range(2)]
        drawn = [add_rows(couple[k] * at_obs) for k in range(3)]
        pushed = [m00 * projected[0] + m01 * projected[1], m01 * projected[0] + m11 * projected[1]]
        pooled = exact_dot(pad_rows(drawn, 8), same_table, 0)
        pooled = [pooled[k : k + 1] for k in range(3)]
        if turn < ITERS:
            image = jc[0] * pushed[0] + jc[1] * pushed[1]
            for k in range(3):
                image = image - couple[k] * pooled[k]
            image = all_reduce(exact_dot(image, cam_table, 1), turn) + direction
            alpha = progress / add_all(direction * image)
        else:
            value = projected[0] * pushed[0] + projected[1] * pushed[1]
            for k in range(3):
                value = value - drawn[k] * pooled[k]
            short = value[:, 0:128]
            for column in range(1, width // 128):
                short = short + value[:, 128 * column : 128 * column + 128]
            short = all_reduce(pad_rows([short], 8), turn)
            alpha = progress / (add_all(short) + add_all(direction * direction))
        solution = solution + alpha * direction
        reached = [reached[k] + alpha * pooled[k] for k in range(3)]
        if turn < ITERS:
            remaining = remaining - alpha * image
            conditioned = precondition(remaining)
            renewed = add_all(remaining * conditioned)
            direction = conditioned + (renewed / progress) * direction
            progress = renewed

    step_ref[...] = solution[:6]
    b2 = reached[2] * i2
    b1 = (reached[1] - l21 * b2) * i1
    b0 = (reached[0] - l10 * b1 - l20 * b2) * i0
    point_ref[...] = -exact_dot(pad_rows([b0, b1, b2], 8), first_table, 1)[:3]


def solve(sizes, terms, cam_jac, pt_jac, obs_camera, point_counts, cameras):
    points = point_counts.shape[1]
    buffers = []
    for turn in range(ITERS + 1):
        rows = 32 if turn == 0 else 8
        columns = cameras if turn < ITERS else 128
        buffers += [pltpu.VMEM((sizes[axis], rows, columns), f32) for axis in AXES]
    semaphores = []
    for axis in AXES:
        semaphores += [pltpu.SemaphoreType.DMA((ITERS + 1, max(sizes[axis] - 1, 1)))] * 2

    def kernel(*refs):
        solver_kernel(sizes, *refs)

    return pl.pallas_call(
        kernel,
        in_specs=[pl.BlockSpec(memory_space=pltpu.VMEM)] * 5,
        out_specs=[pl.BlockSpec(memory_space=pltpu.VMEM)] * 2,
        out_shape=[
            jax.ShapeDtypeStruct((6, cameras), f32),
            jax.ShapeDtypeStruct((3, points), f32),
        ],
        scratch_shapes=buffers + semaphores,
        compiler_params=pltpu.CompilerParams(
            collective_id=0, has_side_effects=True, vmem_limit_bytes=48 * 1024 * 1024
        ),
    )(terms, cam_jac, pt_jac, obs_camera.reshape(1, -1), point_counts)


def solution(mesh):
    sizes = {axis: mesh.shape[axis] for axis in AXES}
    cameras = CAM_DEV * sizes["cam"] * sizes["pts"]

    def shards(feat_res, feat_grad, cam_jac, pt_jac, obs_camera, point_counts):
        terms = features(feat_res, feat_grad)
        return tuple(solve(sizes, terms, cam_jac, pt_jac, obs_camera, point_counts, cameras))

    return jax.shard_map(
        shards,
        mesh=mesh,
        in_specs=(
            P(None, None, ("pts", "cam")),
            P(None, None, None, ("pts", "cam")),
            P(None, None, ("pts", "cam")),
            P(None, None, ("pts", "cam")),
            P(("pts", "cam")),
            P(("pts", "cam"), None),
        ),
        out_specs=(P(), P(None, ("pts", "cam"))),
        check_vma=False,
    )
```

```python
import jax
import jax.numpy as jnp
from jax import lax
from jax.experimental import pallas as pl
from jax.experimental.pallas import tpu as pltpu
from jax.sharding import PartitionSpec as P

CAM_DEV = 8
ITERS = 4
STEPS = 2
PLANS = (("cam", "pts"),) + (("pair", "chips"),) * 4
AXES = ("cam", "pts")
MESH = pl.DeviceIdType.MESH
f32 = jnp.float32
bf16 = jnp.bfloat16


def feature_kernel(res_ref, grad_ref, out_ref, acc_ref):
    step = pl.program_id(0)
    pixels, channels, width = res_ref.shape
    slabs = channels // 16

    @pl.when(step == 0)
    def _():
        acc_ref[...] = jnp.zeros_like(acc_ref)

    def fold(value):
        return value[:8] + value[8:]

    def pixel(index, carry):
        sums = list(carry)
        for slab in range(slabs):
            rows = slice(16 * slab, 16 * slab + 16)
            r = res_ref[index, rows, :].astype(f32)
            gx = grad_ref[0, index, rows, :].astype(f32)
            gy = grad_ref[1, index, rows, :].astype(f32)
            for spot, (one, two) in enumerate(
                ((r, r), (gx, gx), (gx, gy), (gy, gy), (gx, r), (gy, r))
            ):
                sums[spot] = sums[spot] + fold(one * two)
        return tuple(sums)

    sums = lax.fori_loop(0, pixels, pixel, tuple(acc_ref[spot] for spot in range(6)))
    for spot in range(6):
        acc_ref[spot] = sums[spot]

    @pl.when(step == pl.num_programs(0) - 1)
    def _():
        whole = [jnp.sum(acc_ref[spot], axis=0, keepdims=True) for spot in range(6)]
        weight = 1.0 / (1.0 + whole[0] / (pixels * pl.num_programs(0) * channels))
        rows = [value * weight for value in whole[1:]]
        out_ref[...] = jnp.concatenate(rows + [jnp.zeros((3, width), f32)], axis=0)


def features(feat_res, feat_grad):
    pixels, channels, width = feat_res.shape
    return pl.pallas_call(
        feature_kernel,
        grid=(STEPS,),
        in_specs=[
            pl.BlockSpec((pixels // STEPS, channels, width), lambda i: (i, 0, 0)),
            pl.BlockSpec((2, pixels // STEPS, channels, width), lambda i: (0, i, 0, 0)),
        ],
        out_specs=pl.BlockSpec((8, width), lambda i: (0, 0)),
        out_shape=jax.ShapeDtypeStruct((8, width), f32),
        scratch_shapes=[pltpu.VMEM((6, 8, width), f32)],
    )(feat_res, feat_grad)


def exact_dot(value, table, contract):
    rows = value.shape[0]
    high = value.astype(bf16).astype(f32)
    rest = value - high
    middle = rest.astype(bf16).astype(f32)
    pieces = jnp.concatenate([high, middle, rest - middle], axis=0).astype(bf16)
    product = lax.dot_general(
        pieces, table, (((1,), (contract,)), ((), ())), preferred_element_type=f32
    )
    return (product[:rows] + product[rows : 2 * rows]) + product[2 * rows :]


def pad_rows(rows, total):
    have = sum(row.shape[0] for row in rows)
    return jnp.concatenate(rows + [jnp.zeros((total - have, rows[0].shape[1]), f32)], axis=0)


def add_rows(value):
    return jnp.sum(value, axis=0, keepdims=True)


def add_all(value):
    return jnp.sum(jnp.sum(value, axis=0, keepdims=True), axis=1, keepdims=True)


def table_of(mask):
    return jnp.where(mask, 1.0, 0.0).astype(bf16)


def peer_groups(sizes, pair_axis, places):
    other_axis = AXES[1 - AXES.index(pair_axis)]
    half = lax.rem(places[pair_axis], 2)
    partner = places[pair_axis] + 1 - 2 * half
    moved = {
        axis: [places[axis]]
        + [lax.rem(places[axis] + away, sizes[axis]) for away in range(1, sizes[axis])]
        for axis in AXES
    }

    def line(axis):
        return (
            {(axis, away): {axis: moved[axis][away]} for away in range(1, sizes[axis])},
            places[axis],
        )

    chips = {}
    for away in reversed(range(sizes[other_axis])):
        for step in range(0, sizes[pair_axis], 2):
            if away and step:
                name = (other_axis, away, step)
                chips[name] = {other_axis: moved[other_axis][away], pair_axis: moved[pair_axis][step]}
            elif away:
                chips[(other_axis, away)] = {other_axis: moved[other_axis][away]}
            elif step:
                chips[(pair_axis, step)] = {pair_axis: moved[pair_axis][step]}
    slot = places[other_axis] * (sizes[pair_axis] // 2) + lax.div(places[pair_axis], 2)
    return {
        "cam": line("cam"),
        "pts": line("pts"),
        "pair": ({("partner",): {pair_axis: partner}}, half),
        "chips": (chips, slot),
    }


def solver_kernel(sizes, pair_axis, feat_ref, cam_ref, pt_ref, id_ref, count_ref, step_ref, point_ref, *scratch):
    places = {axis: lax.axis_index(axis) for axis in AXES}
    buffers, semaphores = scratch[: 2 * (ITERS + 1)], scratch[2 * (ITERS + 1) :]
    cameras, points, width = step_ref.shape[1], point_ref.shape[1], id_ref.shape[1]

    groups = peer_groups(sizes, pair_axis, places)
    barrier = pltpu.get_barrier_semaphore()
    greeted = {}
    for phases in set(PLANS):
        for offsets, _ in map(groups.get, phases):
            greeted.update(offsets)
    for device in greeted.values():
        pl.semaphore_signal(barrier, inc=1, device_id=device, device_id_type=MESH)

    def all_reduce(value, turn):
        for level, phase in enumerate(PLANS[turn]):
            offsets, me = groups[phase]
            held = buffers[2 * turn + level]
            sent, arrived = semaphores[4 * turn + 2 * level : 4 * turn + 2 * level + 2]
            held[me] = value
            copies = []
            for spot, device in enumerate(offsets.values()):
                copies.append(
                    pltpu.make_async_remote_copy(
                        src_ref=held.at[me],
                        dst_ref=held.at[me],
                        send_sem=sent.at[spot],
                        recv_sem=arrived.at[spot],
                        device_id=device,
                        device_id_type=MESH,
                    )
                )
                copies[-1].start()
            for copy in copies:
                copy.wait_recv()
            value = held[0]
            for position in range(1, held.shape[0]):
                value = value + held[position]
            started.extend(copies)
        return value

    started = []
    cam_table = table_of(lax.broadcasted_iota(jnp.int32, (cameras, width), 0) == id_ref[...])
    counts = count_ref[...].astype(f32)
    upper = lax.broadcasted_iota(jnp.int32, (points, points), 0)
    lower = lax.broadcasted_iota(jnp.int32, (points, points), 1)
    ends = jnp.sum(jnp.where(lower <= upper, counts, 0.0), axis=1, keepdims=True)
    starts = jnp.sum(jnp.where(lower < upper, counts, 0.0), axis=1, keepdims=True)
    spot = lax.broadcasted_iota(jnp.int32, (points, width), 1).astype(f32)
    member = (spot >= starts) & (spot < ends)
    first_table = table_of(spot == starts)
    start_row = add_rows(jnp.where(member, starts, 0.0))
    end_row = add_rows(jnp.where(member, ends, 0.0))
    line = lax.broadcasted_iota(jnp.int32, (width, width), 0).astype(f32)
    same_table = table_of((line >= start_row) & (line < end_row))

    m00, m01, m11, p0, p1 = (feat_ref[row : row + 1, :] for row in range(5))
    jc = [pad_rows([cam_ref[axis]], 8) for axis in range(2)]
    jp = [[pt_ref[axis, row : row + 1, :] for row in range(3)] for axis in range(2)]

    mjp = [
        [m00 * jp[0][k] + m01 * jp[1][k] for k in range(3)],
        [m01 * jp[0][k] + m11 * jp[1][k] for k in range(3)],
    ]
    pairs = [(0, 0), (1, 0), (2, 0), (1, 1), (2, 1), (2, 2)]
    rows = [jp[0][i] * mjp[0][j] + jp[1][i] * mjp[1][j] for i, j in pairs]
    rows += [jp[0][k] * p0 + jp[1][k] * p1 for k in range(3)]
    summed = exact_dot(pad_rows(rows, 16), same_table, 0)
    h00, h10, h20, h11, h21, h22, g0, g1, g2 = (summed[row : row + 1] for row in range(9))
    i0 = 1.0 / jnp.sqrt(h00 + 1.0)
    l10, l20 = h10 * i0, h20 * i0
    i1 = 1.0 / jnp.sqrt((h11 + 1.0) - l10 * l10)
    l21 = (h21 - l20 * l10) * i1
    i2 = 1.0 / jnp.sqrt((h22 + 1.0) - l20 * l20 - l21 * l21)

    def forward(a, b, c):
        a = a * i0
        b = (b - l10 * a) * i1
        return a, b, (c - l20 * a - l21 * b) * i2

    mjc = [m00 * jc[0] + m01 * jc[1], m01 * jc[0] + m11 * jc[1]]
    couple = forward(*(jp[0][k] * mjc[0] + jp[1][k] * mjc[1] for k in range(3)))
    force = forward(g0, g1, g2)

    terms = []
    for row in range(6):
        cut = slice(row, row + 1)
        term = jc[0][cut] * mjc[0] + jc[1][cut] * mjc[1]
        for k in range(3):
            term = term - couple[k][cut] * couple[k]
        terms.append(term)
    term = jc[0] * p0 + jc[1] * p1
    for k in range(3):
        term = term - couple[k] * force[k]
    terms.append(term)
    local = exact_dot(jnp.concatenate(terms, axis=0), cam_table, 1)
    packed = [local[8 * row + row : 8 * row + 6] for row in range(6)] + [local[48:54]]
    packed = jnp.concatenate(packed, axis=0)

    pl.semaphore_wait(barrier, len(greeted))
    total = all_reduce(packed, 0)

    offsets = [0, 6, 11, 15, 18, 20, 21]

    def entry(i, j):
        low, high = min(i, j), max(i, j)
        at = offsets[low] + high - low
        return total[at : at + 1]

    level = lax.broadcasted_iota(jnp.int32, (8, cameras), 0)
    inverse = [
        pad_rows([entry(i, j) for j in range(6)], 8) + jnp.where(level == i, 1.0, 0.0)
        for i in range(6)
    ]
    for k in range(6):
        scale = 1.0 / inverse[k][k : k + 1]
        pivot = jnp.where(level == k, scale, inverse[k] * scale)
        for i in range(6):
            if i != k:
                factor = inverse[i][k : k + 1]
                inverse[i] = jnp.where(level == k, 0.0, inverse[i]) - factor * pivot
        inverse[k] = pivot

    def precondition(value):
        answer = inverse[0] * value[0:1]
        for j in range(1, 6):
            answer = answer + inverse[j] * value[j : j + 1]
        return answer

    remaining = -pad_rows([total[21:27]], 8)
    direction = precondition(remaining)
    progress = add_all(remaining * direction)
    solution = jnp.zeros_like(direction)
    reached = list(force)
    for turn in range(1, ITERS + 1):
        at_obs = exact_dot(direction, cam_table, 0)
        projected = [add_rows(jc[axis] * at_obs) for axis in range(2)]
        drawn = [add_rows(couple[k] * at_obs) for k in range(3)]
        pushed = [m00 * projected[0] + m01 * projected[1], m01 * projected[0] + m11 * projected[1]]
        pooled = exact_dot(pad_rows(drawn, 8), same_table, 0)
        pooled = [pooled[k : k + 1] for k in range(3)]
        if turn < ITERS:
            image = jc[0] * pushed[0] + jc[1] * pushed[1]
            for k in range(3):
                image = image - couple[k] * pooled[k]
            image = all_reduce(exact_dot(image, cam_table, 1)[:6], turn)
            image = pad_rows([image], 8) + direction
            alpha = progress / add_all(direction * image)
        else:
            value = projected[0] * pushed[0] + projected[1] * pushed[1]
            for k in range(3):
                value = value - drawn[k] * pooled[k]
            short = value[:, 0:128]
            for column in range(1, width // 128):
                short = short + value[:, 128 * column : 128 * column + 128]
            short = all_reduce(short, turn)
            alpha = progress / (add_all(short) + add_all(direction * direction))
        solution = solution + alpha * direction
        reached = [reached[k] + alpha * pooled[k] for k in range(3)]
        if turn < ITERS:
            remaining = remaining - alpha * image
            conditioned = precondition(remaining)
            renewed = add_all(remaining * conditioned)
            direction = conditioned + (renewed / progress) * direction
            progress = renewed

    step_ref[...] = solution[:6]
    for copy in started:
        copy.wait_send()
    b2 = reached[2] * i2
    b1 = (reached[1] - l21 * b2) * i1
    b0 = (reached[0] - l10 * b1 - l20 * b2) * i0
    point_ref[...] = -exact_dot(pad_rows([b0, b1, b2], 8), first_table, 1)[:3]


def solve(sizes, pair_axis, terms, cam_jac, pt_jac, obs_camera, point_counts, cameras):
    points = point_counts.shape[1]
    buffers, semaphores = [], []
    chips = sizes["cam"] * sizes["pts"] // 2
    members = {"cam": sizes["cam"], "pts": sizes["pts"], "pair": 2, "chips": chips}
    for turn, phases in enumerate(PLANS):
        rows = 27 if turn == 0 else 6 if turn < ITERS else 1
        columns = cameras if turn < ITERS else 128
        for phase in phases:
            buffers.append(pltpu.VMEM((members[phase], rows, columns), f32))
            semaphores += [pltpu.SemaphoreType.DMA((members[phase] - 1,))] * 2

    def kernel(*refs):
        solver_kernel(sizes, pair_axis, *refs)

    return pl.pallas_call(
        kernel,
        in_specs=[pl.BlockSpec(memory_space=pltpu.VMEM)] * 5,
        out_specs=[pl.BlockSpec(memory_space=pltpu.VMEM)] * 2,
        out_shape=[
            jax.ShapeDtypeStruct((6, cameras), f32),
            jax.ShapeDtypeStruct((3, points), f32),
        ],
        scratch_shapes=buffers + semaphores,
        compiler_params=pltpu.CompilerParams(
            collective_id=0, has_side_effects=True, vmem_limit_bytes=48 * 1024 * 1024
        ),
    )(terms, cam_jac, pt_jac, obs_camera.reshape(1, -1), point_counts)


def chip_axis(mesh):
    for axis in AXES:
        lines = mesh.devices if mesh.axis_names[0] == axis else mesh.devices.T
        spots = [getattr(device, "coords", None) for device in lines[:2, 0]]
        if len(spots) == 2 and spots[0] is not None and list(spots[0]) == list(spots[1]):
            return axis
    return "cam"


def solution(mesh):
    sizes = {axis: mesh.shape[axis] for axis in AXES}
    cameras = CAM_DEV * sizes["cam"] * sizes["pts"]
    pair_axis = chip_axis(mesh)

    def shards(feat_res, feat_grad, cam_jac, pt_jac, obs_camera, point_counts):
        terms = features(feat_res, feat_grad)
        return tuple(solve(sizes, pair_axis, terms, cam_jac, pt_jac, obs_camera, point_counts, cameras))

    return jax.shard_map(
        shards,
        mesh=mesh,
        in_specs=(
            P(None, None, ("pts", "cam")),
            P(None, None, None, ("pts", "cam")),
            P(None, None, ("pts", "cam")),
            P(None, None, ("pts", "cam")),
            P(("pts", "cam")),
            P(("pts", "cam"), None),
        ),
        out_specs=(P(), P(None, ("pts", "cam"))),
        check_vma=False,
    )
```
